32 devices in a mesh: doc: 4 (over y, x), ctx: 8 (over z, core).
Axes of the slice: x: 2, y: 2, z: 4, core: 2. Of those that a mesh axis runs over, the one named last changes fastest.
Arguments:
- summary_cache: bfloat16 [8, 16, 512, 2048], P(None, 'doc', None, 'ctx'), may hold values from -4 to 4
- queries: bfloat16 [4, 2048, 4096], P('doc', 'ctx'), may hold values from -100 to 100
- section_counts: int32 [16], replicated, may hold values from 1 to 2
- summary_blocks: int32 [16, 2], replicated, may hold values from 1 to 2
Outputs:
- attended: bfloat16 [4, 2048, 4096], P('doc', 'ctx')
- relayed: bfloat16 [8, 4, 2048, 2048], P(None, 'doc', 'ctx')
The draws below stay inside these ranges and needn't reach their ends.
All inputs are finite; a program needn't handle non-finite values.
Results may differ from the reference program's by a relative error of at most 0.0045.
Values may be sent and summed in bfloat16 or wider, within the bound.
A program may use at most 192 MiB of HBM per device.

```python
import math
import jax
import jax.numpy as jnp
from jax import lax

QH = 32
KVH = 8
HD = 128
LAYERS = 8
BLOCK = 128
SUMBLK = 2
SECTIONS = 2
GROUP = 4
FEAT = 2048
SUMLEN = 256
SEQD = 512
GROUPS = 4
DOCS = 16
GSEQ = 2048


def draw_summary_cache(key, part):
    array_shape = (LAYERS, DOCS, SEQD, FEAT)
    base_key = jax.random.fold_in(key, 3)
    values = jnp.clip(jax.random.normal(base_key, array_shape, jnp.float32), -4.0, 4.0)
    return values.astype(jnp.bfloat16)


def draw_queries(key, part):
    array_shape = (GROUPS, GSEQ, QH * HD)
    base_key = jax.random.fold_in(key, 5)
    values = jnp.clip(jax.random.normal(base_key, array_shape, jnp.float32), -4.0, 4.0)
    return values.astype(jnp.bfloat16)


def with_ends(values, key, least, largest):
    longest = values.shape.index(max(values.shape))
    spots = []
    for shift in (0, 1):
        where = [jax.random.randint(jax.random.fold_in(key, axis), (), 0, length) for axis, length in enumerate(values.shape)]
        where[longest] = (where[longest] + shift) % values.shape[longest]
        spots.append(tuple(where))
    return values.at[spots[0]].set(least).at[spots[1]].set(largest)


def setup_inputs(seed: int = 0) -> dict:
    arg_keys = jax.random.split(jax.random.key(seed), 5)
    summary_cache = draw_summary_cache(jax.random.fold_in(arg_keys[4], 71), 0)
    queries = draw_queries(jax.random.fold_in(arg_keys[4], 71), 0)
    section_counts = with_ends(jax.random.randint(arg_keys[2], (DOCS,), 1, SECTIONS + 1), jax.random.fold_in(arg_keys[2], 1), 1, SECTIONS).astype(jnp.int32)
    summary_blocks = with_ends(jax.random.randint(arg_keys[3], (DOCS, SECTIONS), 1, SUMBLK + 1), jax.random.fold_in(arg_keys[3], 1), 1, SUMBLK).astype(jnp.int32)
    return dict(summary_cache=summary_cache, queries=queries, section_counts=section_counts, summary_blocks=summary_blocks)


NEGATIVE = -1e+30

def attend_group(operands):
    query_rows, key_rows, validity = operands
    block_rows = min(GSEQ, 512)
    pieces = []
    for offset in range(0, GSEQ, block_rows):
        key_end = offset + block_rows
        grouped = query_rows[offset:key_end].astype(jnp.float32).reshape(block_rows, KVH, GROUP, HD)
        key_heads = key_rows[:key_end, :KVH * HD].astype(jnp.float32).reshape(key_end, KVH, HD)
        value_heads = key_rows[:key_end, KVH * HD:].astype(jnp.float32).reshape(key_end, KVH, HD)
        scores = jnp.einsum('pkgd,skd->kgps', grouped, key_heads) * (1.0 / math.sqrt(HD))
        key_positions = jnp.arange(key_end)
        query_positions = offset + jnp.arange(block_rows)
        allowed = validity[None, :key_end] & (key_positions[None, :] <= query_positions[:, None])
        masked = jnp.where(allowed, scores, NEGATIVE)
        row_maximum = lax.optimization_barrier(jnp.max(masked, axis=-1, keepdims=True))
        weights = jnp.where(allowed, jnp.exp(masked - row_maximum), 0.0)
        denominator = lax.optimization_barrier(jnp.sum(weights, axis=-1))
        rounded = lax.optimization_barrier(weights.astype(jnp.bfloat16)).astype(jnp.float32)
        accumulated = jnp.einsum('kgps,skd->kgpd', rounded, value_heads)
        result = accumulated / denominator[..., None]
        pieces.append(jnp.transpose(result, (2, 0, 1, 3)).reshape(block_rows, QH * HD))
    return jnp.concatenate(pieces, axis=0).astype(jnp.bfloat16)

def reference(summary_cache, queries, section_counts, summary_blocks):
    relayed = jnp.transpose(summary_cache.reshape(LAYERS, GROUPS, GROUPS, SEQD, FEAT), (0, 2, 1, 3, 4)).reshape(LAYERS, GROUPS, GSEQ, FEAT)
    counts_table = jnp.transpose(section_counts.reshape(GROUPS, GROUPS), (1, 0))
    blocks_table = jnp.transpose(summary_blocks.reshape(GROUPS, GROUPS, SECTIONS), (1, 0, 2))
    live_section = jnp.arange(SECTIONS)[None, None, :] < counts_table[:, :, None]
    live_slot = jnp.arange(SUMLEN)[None, None, None, :] < BLOCK * blocks_table[:, :, :, None]
    validity = (live_section[..., None] & live_slot).reshape(GROUPS, GSEQ)
    attended = lax.map(attend_group, (queries, relayed[0], validity))
    return (attended, relayed)
```

```python
import functools
import math

import jax
import jax.numpy as jnp
from jax import lax
from jax.experimental import pallas as pl
from jax.experimental.pallas import tpu as pltpu
from jax.sharding import PartitionSpec as P

QH = 32
KVH = 8
HD = 128
BLOCK = 128
SECTIONS = 2
GROUP = 4
SUMLEN = 256


NEGATIVE = -1e30


MESH = pl.DeviceIdType.MESH


def kernel(
    rows,
    ctx,
    cache,
    queries,
    counts,
    blocks,
    attended,
    relayed,
    kv,
    mid,
    q_vmem,
    out_vmem,
    bias,
    s1,
    r1_first,
    r1,
    up_sem,
    down_sem,
    side_sem,
    kv_sem,
    s2,
    r2,
    local_sem,
):
    layers, _, slots, feat = cache.shape
    own = queries.shape[0]
    pieces = slots // own
    chips = ctx // 2
    me = lax.axis_index("doc")
    c = lax.axis_index("ctx")
    z = c // 2
    core = c % 2
    def seen(chip):
        return ((2 * chip + 2) * own + slots - 1) // slots

    barrier = pltpu.get_barrier_semaphore()
    for k in range(1, rows):
        pl.semaphore_signal(barrier, inc=1, device_id=((me + k) % rows, c), device_id_type=MESH)
    for k in range(1, ctx):
        pl.semaphore_signal(barrier, inc=1, device_id=(me, (c + k) % ctx), device_id_type=MESH)

    own_kv = pltpu.make_async_copy(
        cache.at[0, me], kv.at[c, pl.ds(pl.multiple_of(me * slots, slots), slots)], local_sem.at[0]
    )
    own_kv.start()
    q_copy = pltpu.make_async_copy(queries, q_vmem, local_sem.at[1])
    own_mid = pltpu.make_async_copy(cache.at[pl.ds(1, layers - 1), me], mid.at[:, me], local_sem.at[2])
    pl.semaphore_wait(barrier, rows - 1 + ctx - 1)

    def doc(ref, slice_index, j):
        return ref.at[slice_index, pl.ds(pl.multiple_of(j * slots, slots), slots)]

    def first_copy(j_to, j_from):
        return pltpu.make_async_remote_copy(
            src_ref=cache.at[0, j_to],
            dst_ref=doc(kv, c, j_from),
            send_sem=s1,
            recv_sem=r1_first.at[j_from],
            device_id=(j_to, c),
            device_id_type=MESH,
        )

    for k in range(1, rows):
        first_copy((me + k) % rows, me).start()
    own_mid.start()
    q_copy.start()

    def row_copy(l, j_to):
        return pltpu.make_async_remote_copy(
            src_ref=cache.at[l, j_to],
            dst_ref=mid.at[l - 1, me],
            send_sem=s1,
            recv_sem=r1.at[l],
            device_id=(j_to, c),
            device_id_type=MESH,
        )

    @pl.loop(1, layers)
    def _(l):
        for k in range(1, rows):
            row_copy(l, (me + k) % rows).start()

    def kv_copy(slice_index, j, sems, target):
        return pltpu.make_async_remote_copy(
            src_ref=doc(kv, slice_index, j),
            dst_ref=doc(kv, slice_index, j),
            send_sem=sems.at[slice_index, j],
            recv_sem=kv_sem.at[slice_index, j],
            device_id=(me, target),
            device_id_type=MESH,
        )

    def pass_on(slice_index, j, upward, downward):
        if upward:

            @pl.when(z < chips - 1)
            def _():
                kv_copy(slice_index, j, up_sem, c + 2).start()

        if downward:

            @pl.when((z > 0) & (j < seen(z - 1)))
            def _():
                kv_copy(slice_index, j, down_sem, c - 2).start()

        @pl.when(j < seen(z))
        def _():
            kv_copy(slice_index, j, side_sem, c + 1 - 2 * core).start()

    def spread(l, chosen):
        for k in chosen:
            t = (c + k) % ctx
            j = t // pieces
            h = t % pieces
            pltpu.make_async_remote_copy(
                src_ref=mid.at[l - 1, j, pl.ds(pl.multiple_of(h * own, own), own)],
                dst_ref=relayed.at[l, :, pl.ds(pl.multiple_of(c * feat, feat), feat)],
                send_sem=s2,
                recv_sem=r2,
                device_id=(me, t),
                device_id_type=MESH,
            ).start()

    def layer_step(l):
        arrived = mid.at[l - 1, pl.ds(0, rows - 1)]
        pltpu.make_async_copy(arrived, arrived, r1.at[l]).wait()
        spread(l, range(1, ctx))
        pltpu.make_async_copy(
            mid.at[l - 1, c // pieces, pl.ds(pl.multiple_of((c % pieces) * own, own), own)],
            relayed.at[l, :, pl.ds(pl.multiple_of(c * feat, feat), feat)],
            local_sem.at[3],
        ).start()

    own_kv.wait()
    pass_on(c, me, True, True)
    for k in range(1, rows):
        j = (me + k) % rows
        first_copy(me, j).wait_recv()
        pass_on(c, j, True, True)
    own_mid.wait()
    for step in range(1, chips):

        @pl.when(z >= step)
        def _():
            for k in range(rows):
                j = (me + k) % rows
                kv_copy(c - 2 * step, j, up_sem, c).wait_recv()
                pass_on(c - 2 * step, j, True, False)

        @pl.when(z + step < chips)
        def _():
            for k in range(rows):
                j = (me + k) % rows

                @pl.when(j < seen(z))
                def _():
                    kv_copy(c + 2 * step, j, down_sem, c).wait_recv()
                    pass_on(c + 2 * step, j, False, True)

        layer_step(step)

    @pl.loop(0, seen(z))
    def _(j):
        at = j * rows + me
        key = lax.broadcasted_iota(jnp.int32, (own, slots), 1)
        query = lax.broadcasted_iota(jnp.int32, (own, slots), 0)
        section = key // SUMLEN
        reach = jnp.zeros((own, slots), jnp.int32)
        for s in range(SECTIONS):
            reach = jnp.where((section == s) & (s < counts[at]), BLOCK * blocks[at, s], reach)
        allowed = (key - section * SUMLEN < reach) & (j * slots + key <= c * own + query)
        bias[j] = jnp.where(allowed, 0.0, NEGATIVE)

    for other in range(chips):
        slice_index = 2 * other + 1 - core

        @pl.loop(0, seen(z))
        def _(j):
            kv_copy(slice_index, j, side_sem, c).wait_recv()

    q_copy.wait()
    for t in range(ctx):
        pltpu.make_async_copy(
            kv.at[t, pl.ds(pl.multiple_of(c * own, own), own)],
            relayed.at[0, :, pl.ds(t * feat, feat)],
            local_sem.at[4],
        ).start()

    factor = math.log2(math.e) / math.sqrt(HD)

    @pl.loop(0, KVH)
    def _(k):
        @pl.when(k + chips < layers)
        def _():
            layer_step(k + chips)

        per = feat // HD
        key_slice = k // per
        value_slice = (KVH + k) // per
        lanes = pl.ds(pl.multiple_of((k % per) * HD, HD), HD)
        for i in range(GROUP):
            column = pl.ds(pl.multiple_of((k * GROUP + i) * HD, HD), HD)
            q = q_vmem[:, column]

            def block(j, state):
                top, total, acc = state
                at = pl.ds(pl.multiple_of(j * slots, slots), slots)
                s = lax.dot_general(
                    q, kv[key_slice, at, lanes], (((1,), (1,)), ((), ())), preferred_element_type=jnp.float32
                )
                s = s + bias[j]
                newest = jnp.maximum(top, jnp.max(s, axis=1, keepdims=True))
                w = jnp.exp2((s - newest) * factor)
                shrink = jnp.exp2((top - newest) * factor)
                total = total * shrink + jnp.sum(w, axis=1, keepdims=True)
                acc = acc * shrink + jnp.dot(
                    w.astype(jnp.bfloat16), kv[value_slice, at, lanes], preferred_element_type=jnp.float32
                )
                return newest, total, acc

            start = (
                jnp.full((own, 1), NEGATIVE, jnp.float32),
                jnp.zeros((own, 1), jnp.float32),
                jnp.zeros((own, HD), jnp.float32),
            )
            _, total, acc = lax.fori_loop(0, seen(z), block, start)
            out_vmem[:, column] = (acc / total).astype(jnp.bfloat16)

    out_copy = pltpu.make_async_copy(out_vmem, attended, local_sem.at[1])
    out_copy.start()

    @pl.loop(0, ctx)
    def _(t):
        @pl.loop(0, rows)
        def _(j):
            @pl.when(t % 2 == core)
            def _():
                chip = t // 2

                @pl.when((z < chips - 1) & (chip <= z))
                def _():
                    kv_copy(t, j, up_sem, c).wait_send()

                @pl.when((z > 0) & (j < seen(z - 1)) & (chip >= z))
                def _():
                    kv_copy(t, j, down_sem, c).wait_send()

                @pl.when(j < seen(z))
                def _():
                    kv_copy(t, j, side_sem, c).wait_send()

    def sized(ref, sem):
        return pltpu.make_async_copy(ref, ref, sem)

    sized(cache.at[:, pl.ds(0, rows - 1)], s1).wait()
    passed = relayed.at[pl.ds(1, layers - 1), :, pl.ds(0, (ctx - 1) * feat)]
    sized(passed, s2).wait()
    sized(passed, r2).wait()
    sized(relayed.at[pl.ds(1, layers - 1), :, pl.ds(0, feat)], local_sem.at[3]).wait()
    sized(relayed.at[0], local_sem.at[4]).wait()
    out_copy.wait()


def local(summary_cache, queries, section_counts, summary_blocks):
    rows = lax.axis_size("doc")
    ctx = lax.axis_size("ctx")
    layers, documents, slots, feat = summary_cache.shape
    own = queries.shape[1]
    dtype = summary_cache.dtype
    any_space = pl.BlockSpec(memory_space=pl.ANY)
    scalars = pl.BlockSpec(memory_space=pltpu.SMEM)
    dma = pltpu.SemaphoreType.DMA
    attended, relayed = pl.pallas_call(
        functools.partial(kernel, rows, ctx),
        out_shape=(
            jax.ShapeDtypeStruct(queries.shape[1:], dtype),
            jax.ShapeDtypeStruct((layers, own, ctx * feat), dtype),
        ),
        in_specs=[any_space, any_space, scalars, scalars],
        out_specs=(any_space, any_space),
        scratch_shapes=[
            pltpu.VMEM((ctx, rows * slots, feat), dtype),
            pltpu.VMEM((layers - 1, rows, slots, feat), dtype),
            pltpu.VMEM(queries.shape[1:], dtype),
            pltpu.VMEM(queries.shape[1:], dtype),
            pltpu.VMEM((rows, own, slots), jnp.float32),
            dma,
            dma((rows,)),
            dma((layers,)),
            dma((ctx, rows)),
            dma((ctx, rows)),
            dma((ctx, rows)),
            dma((ctx, rows)),
            dma,
            dma,
            dma((5,)),
        ],
        compiler_params=pltpu.CompilerParams(
            collective_id=0, has_side_effects=True, vmem_limit_bytes=60 * 1024 * 1024
        ),
    )(summary_cache, queries[0], section_counts, summary_blocks)
    return attended[None], relayed[:, None]


def solution(mesh):
    placed = (P(None, "doc", None, "ctx"), P("doc", "ctx", None), P(), P())
    return jax.shard_map(
        local,
        mesh=mesh,
        in_specs=placed,
        out_specs=(P("doc", "ctx", None), P(None, "doc", "ctx", None)),
        check_vma=False,
    )
```

```python
import functools
import math

import jax
import jax.numpy as jnp
from jax import lax
from jax.experimental import pallas as pl
from jax.experimental.pallas import tpu as pltpu
from jax.sharding import PartitionSpec as P

QH = 32
KVH = 8
HD = 128
BLOCK = 128
SECTIONS = 2
GROUP = 4
SUMLEN = 256


NEGATIVE = -1e30


MESH = pl.DeviceIdType.MESH


def kernel(
    rows,
    ctx,
    cache,
    queries,
    counts,
    blocks,
    attended,
    relayed,
    kv,
    mid,
    q_vmem,
    out_vmem,
    bias,
    s1,
    r1_first,
    r1,
    up_sem,
    down_sem,
    side_sem,
    kv_sem,
    s2,
    r2,
    local_sem,
):
    layers, _, slots, feat = cache.shape
    own = queries.shape[0]
    pieces = slots // own
    chips = ctx // 2
    me = lax.axis_index("doc")
    c = lax.axis_index("ctx")
    z = c // 2
    core = c % 2
    def partner(k):
        if rows & (rows - 1):
            return (me + k) % rows
        row, bit = me, 1
        while bit < rows:
            if k & bit:
                row = row + bit * (1 - 2 * ((me // bit) % 2))
            bit *= 2
        return row

    def seen(chip):
        return ((2 * chip + 2) * own + slots - 1) // slots

    barrier = pltpu.get_barrier_semaphore()
    for k in range(1, rows):
        pl.semaphore_signal(barrier, inc=1, device_id=(partner(k), c), device_id_type=MESH)
    for k in range(1, ctx):
        pl.semaphore_signal(barrier, inc=1, device_id=(me, (c + k) % ctx), device_id_type=MESH)

    own_kv = pltpu.make_async_copy(
        cache.at[0, me], kv.at[c, pl.ds(pl.multiple_of(me * slots, slots), slots)], local_sem.at[0]
    )
    own_kv.start()
    q_copy = pltpu.make_async_copy(queries, q_vmem, local_sem.at[1])
    own_mid = pltpu.make_async_copy(cache.at[pl.ds(1, layers - 1), me], mid.at[:, me], local_sem.at[2])
    pl.semaphore_wait(barrier, rows - 1 + ctx - 1)

    def doc(ref, slice_index, j):
        return ref.at[slice_index, pl.ds(pl.multiple_of(j * slots, slots), slots)]

    def first_copy(j_to, j_from):
        return pltpu.make_async_remote_copy(
            src_ref=cache.at[0, j_to],
            dst_ref=doc(kv, c, j_from),
            send_sem=s1,
            recv_sem=r1_first.at[j_from],
            device_id=(j_to, c),
            device_id_type=MESH,
        )

    for k in range(1, rows):
        first_copy(partner(k), me).start()
    own_mid.start()
    q_copy.start()

    def row_copy(l, j_to):
        return pltpu.make_async_remote_copy(
            src_ref=cache.at[l, j_to],
            dst_ref=mid.at[l - 1, me],
            send_sem=s1,
            recv_sem=r1.at[l],
            device_id=(j_to, c),
            device_id_type=MESH,
        )

    @pl.loop(1, layers)
    def _(l):
        for k in range(1, rows):
            row_copy(l, partner(k)).start()

    def kv_copy(slice_index, j, sems, target):
        return pltpu.make_async_remote_copy(
            src_ref=doc(kv, slice_index, j),
            dst_ref=doc(kv, slice_index, j),
            send_sem=sems.at[slice_index, j],
            recv_sem=kv_sem.at[slice_index, j],
            device_id=(me, target),
            device_id_type=MESH,
        )

    def pass_on(slice_index, j, upward, downward):
        if upward:

            @pl.when(z < chips - 1)
            def _():
                kv_copy(slice_index, j, up_sem, c + 2).start()

        if downward:

            @pl.when((z > 0) & (j < seen(z - 1)))
            def _():
                kv_copy(slice_index, j, down_sem, c - 2).start()

        @pl.when(j < seen(z))
        def _():
            kv_copy(slice_index, j, side_sem, c + 1 - 2 * core).start()

    def send_piece(l, t):
        j = t // pieces
        h = t % pieces
        pltpu.make_async_remote_copy(
            src_ref=mid.at[l - 1, j, pl.ds(pl.multiple_of(h * own, own), own)],
            dst_ref=relayed.at[l, :, pl.ds(pl.multiple_of(c * feat, feat), feat)],
            send_sem=s2,
            recv_sem=r2,
            device_id=(me, t),
            device_id_type=MESH,
        ).start()

    def spread(l, distances):
        for d in distances:
            for other in (core, 1 - core):

                @pl.when(z + d < chips)
                def _():
                    send_piece(l, 2 * (z + d) + other)

                @pl.when(z >= d)
                def _():
                    send_piece(l, 2 * (z - d) + other)

    def layer_step(l):
        if l < layers:
            arrived = mid.at[l - 1, pl.ds(0, rows - 1)]
            pltpu.make_async_copy(arrived, arrived, r1.at[l]).wait()
        for d in range(1, chips):
            late = l - (d - 1)
            if 0 < late < layers:
                spread(late, [d])
        if l < layers:
            send_piece(l, c + 1 - 2 * core)
            pltpu.make_async_copy(
                mid.at[l - 1, c // pieces, pl.ds(pl.multiple_of((c % pieces) * own, own), own)],
                relayed.at[l, :, pl.ds(pl.multiple_of(c * feat, feat), feat)],
                local_sem.at[3],
            ).start()

    own_kv.wait()
    pass_on(c, me, True, True)
    for k in range(1, rows):
        j = partner(k)
        first_copy(me, j).wait_recv()
        pass_on(c, j, True, True)
    own_mid.wait()
    next_step = 1
    for step in range(1, chips):

        @pl.when(z >= step)
        def _():
            for k in range(rows):
                j = partner(k)
                kv_copy(c - 2 * step, j, up_sem, c).wait_recv()
                pass_on(c - 2 * step, j, True, False)

        @pl.when(z + step < chips)
        def _():
            for k in range(rows):
                j = partner(k)

                @pl.when(j < seen(z))
                def _():
                    kv_copy(c + 2 * step, j, down_sem, c).wait_recv()
                    pass_on(c + 2 * step, j, False, True)

        for _ in range(2):
            layer_step(next_step)
            next_step += 1

    @pl.loop(0, seen(z))
    def _(j):
        at = j * rows + me
        key = lax.broadcasted_iota(jnp.int32, (own, slots), 1)
        query = lax.broadcasted_iota(jnp.int32, (own, slots), 0)
        section = key // SUMLEN
        reach = jnp.zeros((own, slots), jnp.int32)
        for s in range(SECTIONS):
            reach = jnp.where((section == s) & (s < counts[at]), BLOCK * blocks[s, at], reach)
        allowed = (key - section * SUMLEN < reach) & (j * slots + key <= c * own + query)
        bias[j] = jnp.where(allowed, 0.0, NEGATIVE)

    for other in range(chips):
        slice_index = 2 * other + 1 - core

        @pl.loop(0, seen(z))
        def _(j):
            kv_copy(slice_index, j, side_sem, c).wait_recv()

    q_copy.wait()
    for t in range(ctx):
        pltpu.make_async_copy(
            kv.at[t, pl.ds(pl.multiple_of(c * own, own), own)],
            relayed.at[0, :, pl.ds(t * feat, feat)],
            local_sem.at[4],
        ).start()

    factor = math.log2(math.e) / math.sqrt(HD)

    last_step = layers + chips - 2

    @pl.loop(0, KVH)
    def _(k):
        for l in range(next_step, last_step):

            @pl.when(k == l - next_step)
            def _():
                layer_step(l)

        per = feat // HD
        key_slice = k // per
        value_slice = (KVH + k) // per
        lanes = pl.ds(pl.multiple_of((k % per) * HD, HD), HD)
        for i in range(GROUP):
            column = pl.ds(pl.multiple_of((k * GROUP + i) * HD, HD), HD)
            q = q_vmem[:, column]

            def block(j, state):
                top, total, acc = state
                at = pl.ds(pl.multiple_of(j * slots, slots), slots)
                s = lax.dot_general(
                    q, kv[key_slice, at, lanes], (((1,), (1,)), ((), ())), preferred_element_type=jnp.float32
                )
                s = s + bias[j]
                newest = jnp.maximum(top, jnp.max(s, axis=1, keepdims=True))
                w = jnp.exp2((s - newest) * factor)
                shrink = jnp.exp2((top - newest) * factor)
                total = total * shrink + jnp.sum(w, axis=1, keepdims=True)
                acc = acc * shrink + jnp.dot(
                    w.astype(jnp.bfloat16), kv[value_slice, at, lanes], preferred_element_type=jnp.float32
                )
                return newest, total, acc

            start = (
                jnp.full((own, 1), NEGATIVE, jnp.float32),
                jnp.zeros((own, 1), jnp.float32),
                jnp.zeros((own, HD), jnp.float32),
            )
            _, total, acc = lax.fori_loop(0, seen(z), block, start)
            out_vmem[:, column] = (acc / total).astype(jnp.bfloat16)

    out_copy = pltpu.make_async_copy(out_vmem, attended, local_sem.at[1])
    out_copy.start()

    @pl.loop(0, ctx)
    def _(t):
        @pl.loop(0, rows)
        def _(j):
            @pl.when(t % 2 == core)
            def _():
                chip = t // 2

                @pl.when((z < chips - 1) & (chip <= z))
                def _():
                    kv_copy(t, j, up_sem, c).wait_send()

                @pl.when((z > 0) & (j < seen(z - 1)) & (chip >= z))
                def _():
                    kv_copy(t, j, down_sem, c).wait_send()

                @pl.when(j < seen(z))
                def _():
                    kv_copy(t, j, side_sem, c).wait_send()

    def sized(ref, sem):
        return pltpu.make_async_copy(ref, ref, sem)

    sized(cache.at[:, pl.ds(0, rows - 1)], s1).wait()
    passed = relayed.at[pl.ds(1, layers - 1), :, pl.ds(0, (ctx - 1) * feat)]
    sized(passed, s2).wait()
    sized(passed, r2).wait()
    sized(relayed.at[pl.ds(1, layers - 1), :, pl.ds(0, feat)], local_sem.at[3]).wait()
    sized(relayed.at[0], local_sem.at[4]).wait()
    out_copy.wait()


def copy_out(attended, relayed, attended_out, relayed_out, sems):
    layers = relayed.shape[0]
    copies = [pltpu.make_async_copy(relayed.at[l], relayed_out.at[l], sems.at[l]) for l in range(layers)]
    copies.append(pltpu.make_async_copy(attended, attended_out, sems.at[layers]))
    for copy in copies:
        copy.start()
    for copy in copies:
        copy.wait()


def deliver(attended, relayed):
    any_space = pl.BlockSpec(memory_space=pl.ANY)
    return pl.pallas_call(
        copy_out,
        out_shape=(
            jax.ShapeDtypeStruct(attended.shape, attended.dtype),
            jax.ShapeDtypeStruct(relayed.shape, relayed.dtype),
        ),
        in_specs=[any_space, any_space],
        out_specs=(any_space, any_space),
        scratch_shapes=[pltpu.SemaphoreType.DMA((relayed.shape[0] + 1,))],
        compiler_params=pltpu.CompilerParams(vmem_limit_bytes=4 * 1024 * 1024),
    )(attended, relayed)


def local(summary_cache, queries, section_counts, summary_blocks):
    rows = lax.axis_size("doc")
    ctx = lax.axis_size("ctx")
    layers, documents, slots, feat = summary_cache.shape
    own = queries.shape[1]
    dtype = summary_cache.dtype
    any_space = pl.BlockSpec(memory_space=pl.ANY)
    held = pl.BlockSpec(memory_space=pltpu.HBM)
    scalars = pl.BlockSpec(memory_space=pltpu.SMEM)
    dma = pltpu.SemaphoreType.DMA
    size = rows * slots * feat * (ctx + layers - 1) * 2 + own * queries.shape[2] * 4 + rows * own * slots * 4
    room = size + own * (layers * ctx * feat + queries.shape[2]) * 2 + 4 * 1024 * 1024
    place = pltpu.VMEM if room < 60 * 1024 * 1024 else pltpu.HBM

    def in_hbm(array):
        return pltpu.with_memory_space_constraint(array, pltpu.HBM)

    attended, relayed = pl.pallas_call(
        functools.partial(kernel, rows, ctx),
        out_shape=(
            place(queries.shape[1:], dtype),
            place((layers, own, ctx * feat), dtype),
        ),
        in_specs=[held, held, scalars, scalars],
        out_specs=(any_space, any_space),
        scratch_shapes=[
            pltpu.VMEM((ctx, rows * slots, feat), dtype),
            pltpu.VMEM((layers - 1, rows, slots, feat), dtype),
            pltpu.VMEM(queries.shape[1:], dtype),
            pltpu.VMEM(queries.shape[1:], dtype),
            pltpu.VMEM((rows, own, slots), jnp.float32),
            dma,
            dma((rows,)),
            dma((layers,)),
            dma((ctx, rows)),
            dma((ctx, rows)),
            dma((ctx, rows)),
            dma((ctx, rows)),
            dma,
            dma,
            dma((5,)),
        ],
        compiler_params=pltpu.CompilerParams(
            collective_id=0, has_side_effects=True, vmem_limit_bytes=size + 3 * 1024 * 1024
        ),
    )(*(in_hbm(x) for x in (summary_cache, queries[0], section_counts, summary_blocks.T)))
    return deliver(attended[None], relayed[:, None])


def solution(mesh):
    placed = (P(None, "doc", None, "ctx"), P("doc", "ctx", None), P(), P())
    return jax.shard_map(
        local,
        mesh=mesh,
        in_specs=placed,
        out_specs=(P("doc", "ctx", None), P(None, "doc", "ctx", None)),
        check_vma=False,
    )
```
